1024 devices in a mesh: gx: 128 (over z, y), gy: 8 (over x, core).
Axes of the slice: x: 4, y: 4, z: 32, core: 2. Of those that a mesh axis runs over, the one named last changes fastest.
Arguments:
- residual_block: float32 [8, 512, 64, 256], P(None, 'gx', 'gy'), may hold values from -70 to 70
- diagonal: float32 [512, 64, 256], P('gx', 'gy'), may hold values from 0.5 to 4
Outputs:
- correction: float32 [8, 512, 64, 256], P(None, 'gx', 'gy')
- new_residual: float32 [8, 512, 64, 256], P(None, 'gx', 'gy')
- estimate: float32 [8], replicated
The draws below stay inside these ranges and needn't reach their ends.
All inputs are finite; a program needn't handle non-finite values.
Results may differ from the reference program's by a relative error of at most 0.008.
Values sent between devices are 32-bit elements; how exact they have to be, the bound alone decides.
No kernel may reach another device: no remote copies, remote signals or barrier semaphores. Data moves between devices by JAX's collectives and lax.ppermute only.
A program may use at most 32 MiB of HBM per device.

```python
import math
import jax
import jax.numpy as jnp
import numpy as np
from jax import lax

NRHS = 8
NX = 512
NY = 64
NZ = 256


def draw_residual_block(key, part):
    third = jax.random.fold_in(jax.random.fold_in(key, 17), 2)
    coord_x = jnp.arange(NX, dtype=jnp.float32) / NX
    rising = jnp.exp(math.log(3.0) * coord_x)[None, :, None, None]
    values = jnp.clip(jax.random.normal(third, (NRHS, NX, NY, NZ), jnp.float32), -4.0, 4.0)
    return (values * rising).astype(jnp.float32)


def level_of(own_key, shape, cuts, low, top_value):
    factor_of, own = 1.0, jax.random.fold_in(own_key, 6)
    for position, shards_of in cuts:
        heights = jnp.exp(jax.random.uniform(jax.random.fold_in(own, position), (shards_of,), jnp.float32, low / len(cuts), top_value / len(cuts)))
        factor_of = factor_of * jnp.repeat(heights, shape[position] // shards_of).reshape([-1 if axis == position else 1 for axis in range(len(shape))])
    return factor_of


def setup_inputs(seed: int = 0) -> dict:
    streams_of = jax.random.split(jax.random.key(seed), 3)
    residual_block = draw_residual_block(jax.random.fold_in(streams_of[2], 71), 0)
    diagonal = jnp.clip(jnp.exp(math.log(4.0) - 2.0794415 * jax.random.uniform(streams_of[1], (NX, NY, NZ), jnp.float32) ** level_of(streams_of[1], (NX, NY, NZ), ((0, 128), (1, 8)), -0.2, 0.2)), 0.5, 4.0)
    return {"residual_block": residual_block, "diagonal": diagonal}


WEIGHT_X = 0.4
WEIGHT_Y = 0.2
WEIGHT_Z = 0.1
CENTRE = 2.2
SCALE_POWER = 3.0
SHIFTS = (6.0, 1.5, 4.5, 3.0)
EPSILON = 1e-06

def apply_padded(padded, diag_inner, shift_now):
    along_z = jnp.pad(padded, ((0, 0), (0, 0), (0, 0), (1, 1)))
    sum_z = padded + WEIGHT_Z * (along_z[..., :-2] + along_z[..., 2:])
    sum_y = sum_z[:, :, 1:-1] + WEIGHT_Y * (sum_z[:, :, :-2] + sum_z[:, :, 2:])
    sum_x = sum_y[:, 1:-1] + WEIGHT_X * (sum_y[:, :-2] + sum_y[:, 2:])
    centre_cells = padded[:, 1:-1, 1:-1]
    return ((CENTRE + 1.0 + diag_inner - shift_now) * centre_cells - sum_x) / SCALE_POWER

def newton_table():
    blocks = len(SHIFTS)
    identity = np.eye(NRHS, dtype=np.float32)
    matrix = np.zeros(((blocks + 1) * NRHS, blocks * NRHS), np.float32)
    for block_index in range(blocks):
        low = block_index * NRHS
        matrix[low:low + NRHS, low:low + NRHS] = SHIFTS[block_index] * identity
        matrix[low + NRHS:low + 2 * NRHS, low:low + NRHS] = SCALE_POWER * identity
    return matrix

def solve_small(gram_full):
    highest = lax.Precision.HIGHEST
    newton = jnp.asarray(newton_table(), gram_full.dtype)
    image = jnp.dot(newton.T, jnp.dot(gram_full, newton, precision=highest), precision=highest)
    right_side = jnp.dot(newton.T, gram_full[:, :NRHS], precision=highest)
    scales = lax.rsqrt(jnp.diagonal(image) + EPSILON)
    scaled = image * scales[:, None] * scales[None, :]
    factor = jnp.linalg.cholesky(scaled)
    coeffs = scales[:, None] * jax.scipy.linalg.cho_solve((factor, True), scales[:, None] * right_side)
    initial_sq = jnp.diagonal(gram_full)[:NRHS]
    estimate = (initial_sq - lax.optimization_barrier(jnp.sum(right_side * coeffs, axis=0))) / initial_sq
    return (coeffs, jnp.dot(newton, coeffs, precision=highest), estimate)

def reference(residual_block, diagonal):
    highest = lax.Precision.HIGHEST
    powers = [residual_block]
    field_now = residual_block
    for shift_now in SHIFTS:
        padded = jnp.pad(field_now, ((0, 0), (1, 1), (1, 1), (0, 0)))
        field_now = apply_padded(padded, diagonal, shift_now)
        powers.append(field_now)
    basis = jnp.concatenate(powers, 0).reshape(len(powers) * NRHS, -1)
    gram_full = lax.dot_general(basis.astype(jnp.float32), basis.astype(jnp.float32), (((1,), (1,)), ((), ())), precision=highest, preferred_element_type=jnp.float32)
    coeffs, combined, estimate = solve_small(gram_full)
    kept = len(SHIFTS) * NRHS
    correction = lax.dot_general(coeffs.astype(jnp.float32), basis[:kept].astype(jnp.float32), (((0,), (0,)), ((), ())), precision=highest, preferred_element_type=jnp.float32)
    removed = lax.dot_general(combined.astype(jnp.float32), basis.astype(jnp.float32), (((0,), (0,)), ((), ())), precision=highest, preferred_element_type=jnp.float32)
    new_residual = residual_block - removed.reshape(residual_block.shape)
    return (correction.reshape(residual_block.shape), new_residual, estimate)
```

```python
import functools

import jax
import jax.numpy as jnp
import numpy as np
from jax import lax
from jax.experimental import pallas as pl
from jax.experimental.pallas import tpu as pltpu
from jax.sharding import Mesh
from jax.sharding import PartitionSpec as P

NRHS = 8
WEIGHT_X = 0.4
WEIGHT_Y = 0.2
WEIGHT_Z = 0.1
CENTRE = 2.2
SCALE_POWER = 3.0
SHIFTS = (6.0, 1.5, 4.5, 3.0)
DEPTH = len(SHIFTS)

CX, CY, CZ = 4, 8, 256
WX, WY = CX + 2 * DEPTH, CY + 2 * DEPTH
LANES = 128
HIGHEST = lax.Precision.HIGHEST

GX = ("z1", "z0", "y")
NEAR = ("z0", "y", "gy")
FAR = ("z1",)
OWN = CX * CY
PACK = OWN + CX
SIDE = WX * DEPTH
SIDE_PACK = SIDE + WX // 2


def moment_terms():
    table = {}
    for j in range(DEPTH + 1):
        for i in (j, j + 1):
            if i <= DEPTH:
                table[i, j] = np.eye(9)[2 * j + (i - j)]
    for gap in range(2, DEPTH + 1):
        for j in range(DEPTH + 1 - gap):
            i = j + gap - 1
            low = table[i, j + 1]
            table[i + 1, j] = low + (SHIFTS[j] - SHIFTS[i]) / SCALE_POWER * table[i, j]

    def block(i, j):
        return table[max(i, j), min(i, j)]

    alpha = np.zeros((9, DEPTH, DEPTH + 1))
    for i in range(DEPTH):
        for j in range(DEPTH):
            alpha[:, i, j] = (
                SHIFTS[i] * SHIFTS[j] * block(i, j)
                + SCALE_POWER * SHIFTS[i] * block(i, j + 1)
                + SCALE_POWER * SHIFTS[j] * block(i + 1, j)
                + SCALE_POWER**2 * block(i + 1, j + 1)
            )
        alpha[:, i, DEPTH] = SHIFTS[i] * block(i, 0) + SCALE_POWER * block(i + 1, 0)
    return alpha


ROLLS = range(-8, DEPTH + 1)


def roll_table():
    alpha = moment_terms()
    out = np.zeros((DEPTH * len(ROLLS), LANES), np.float32)
    for i in range(DEPTH):
        for k, d in enumerate(ROLLS):
            for j in range(DEPTH + 1):
                if 0 <= j - d < 9:
                    out[i * len(ROLLS) + k, 8 * j : 8 * j + 8] = alpha[j - d, i, j]
    return out


def pack_kernel(res_ref, diag_ref, out_ref):
    for x in range(CX):
        out_ref[CY * x : CY * x + CY] = jnp.swapaxes(res_ref[:, x], 0, 1)
        out_ref[OWN + x] = diag_ref[x]


def side_kernel(par_ref, own_ref, even_ref, odd_ref, die_ref, link_ref):
    px, core = par_ref[0], par_ref[1]
    first = (DEPTH * (1 - core), DEPTH * core)
    row = lax.broadcasted_iota(jnp.int32, (CY, CZ), 0)
    for ref, base in ((own_ref, DEPTH), (even_ref, 8 * (1 - px)), (odd_ref, 8 * px)):
        for x in range(CX):
            for k in range(DEPTH):
                at = (base + x) * DEPTH + k
                die_ref[at] = ref[CY * x + first[0] + k]
                link_ref[at] = ref[CY * x + first[1] + k]
        for k in range(CX // 2):
            a, b = ref[OWN + 2 * k], ref[OWN + 2 * k + 1]
            top = jnp.where(row < 4, a, pltpu.roll(b, 4, 0))
            bottom = jnp.where(row < 4, pltpu.roll(a, 4, 0), b)
            at = SIDE + base // 2 + k
            die_ref[at] = jnp.where(core == 0, bottom, top)
            link_ref[at] = jnp.where(core == 0, top, bottom)


def basis_kernel(
    par_ref, own_ref, even_ref, odd_ref, die_ref, link_ref, v_ref, gram_ref, e0, e1, e2, e3, dm, bc
):
    px, core = par_ref[0], par_ref[1]
    third = 1.0 / SCALE_POWER
    for ref, base in ((own_ref, DEPTH), (even_ref, 8 * (1 - px)), (odd_ref, 8 * px)):
        for x in range(CX):
            for y in range(CY):
                e0[(base + x) * WY + DEPTH + y] = ref[CY * x + y]
            dm[base + x, DEPTH : DEPTH + CY] = ref[OWN + x]
    for ref, base in ((die_ref, 12 * (1 - core)), (link_ref, 12 * core)):
        for x in range(WX):
            for k in range(DEPTH):
                e0[x * WY + base + k] = ref[x * DEPTH + k]

    for low, high, test in ((link_ref, die_ref, core == 0), (die_ref, link_ref, core == 1)):

        @pl.when(test)
        def _(low=low, high=high):
            for k in range(WX // 2):
                for ref, at in ((low, 0), (high, DEPTH + CY)):
                    dm[2 * k, at : at + DEPTH] = ref[SIDE + k, :DEPTH]
                    dm[2 * k + 1, at : at + DEPTH] = ref[SIDE + k, DEPTH:]

    @pl.loop(1, WY - 1)
    def _(y):
        for x in range(1, WX - 1):
            line = (dm[x, pl.ds(y, 1), :] + (CENTRE + 1.0)) * third
            bc[x * WY + y] = jnp.broadcast_to(line, (NRHS, CZ))

    lane = lax.broadcasted_iota(jnp.int32, (NRHS, LANES), 1)
    scratch = (e0, e1, e2, e3)

    def place(level, x):
        if level and DEPTH <= x < DEPTH + CX:
            return v_ref.at[level - 1], (x - DEPTH) * WY
        return scratch[level], x * WY

    for level, shift in enumerate(SHIFTS):
        margin = level + 1

        @pl.loop(margin, WY - margin)
        def _(y, level=level, shift=shift, margin=margin):
            centre, total = {}, {}
            for x in range(level, WX - level):
                ref, at = place(level, x)
                centre[x] = ref[at + y]
                total[x] = centre[x] + WEIGHT_Y * (ref[at + y - 1] + ref[at + y + 1])
            for x in range(margin, WX - margin):
                t = total[x] + WEIGHT_X * (total[x - 1] + total[x + 1])
                a, b = t[:, :LANES], t[:, LANES:]
                up_a, up_b = pltpu.roll(a, 1, 1), pltpu.roll(b, 1, 1)
                dn_a, dn_b = pltpu.roll(a, LANES - 1, 1), pltpu.roll(b, LANES - 1, 1)
                near_a = jnp.where(lane == 0, 0.0, up_a) + jnp.where(lane == LANES - 1, dn_b, dn_a)
                near_b = jnp.where(lane == 0, up_a, up_b) + jnp.where(lane == LANES - 1, 0.0, dn_b)
                coeff = bc[x * WY + y] - shift * third
                new_a = coeff[:, :LANES] * centre[x][:, :LANES] - third * (a + WEIGHT_Z * near_a)
                new_b = coeff[:, LANES:] * centre[x][:, LANES:] - third * (b + WEIGHT_Z * near_b)
                ref, at = place(level + 1, x)
                ref[at + y, :, :LANES] = new_a
                ref[at + y, :, LANES:] = new_b

        if level < DEPTH - 1:
            zero = jnp.zeros((NRHS, CZ), jnp.float32)

            def clear(xs, ys, level=level):
                @pl.loop(ys[0], ys[1])
                def _(y):
                    for x in range(*xs):
                        ref, at = place(level + 1, x)
                        ref[at + y] = zero

            for index, xs, ys in (
                (2, (margin, DEPTH), (margin, WY - margin)),
                (3, (DEPTH + CX, WX - margin), (margin, WY - margin)),
                (4, (margin, WX - margin), (margin, DEPTH)),
                (5, (margin, WX - margin), (DEPTH + CY, WY - margin)),
            ):
                pl.when(par_ref[index] == 1)(functools.partial(clear, xs, ys))

    def add(x, total):
        for y in range(CY):
            parts = [own_ref[x * CY + y]]
            parts += [v_ref[j, x * WY + DEPTH + y] for j in range(DEPTH)]
            w = jnp.concatenate(parts, 0)
            total += lax.dot_general(
                w, w, (((1,), (1,)), ((), ())), precision=HIGHEST, preferred_element_type=jnp.float32
            )
        return total

    count = (DEPTH + 1) * NRHS
    gram = lax.fori_loop(0, CX, add, jnp.zeros((count, count), jnp.float32))
    gram = jnp.concatenate([gram, jnp.zeros((count, LANES - count), jnp.float32)], 1)
    out = jnp.zeros((NRHS, LANES), jnp.float32)
    for i in range(DEPTH + 1):
        mine = pltpu.roll(gram[8 * i : 8 * i + 8], 8 * i, 1) if i else gram[:8]
        out += jnp.where((lane >= 16 * i - 8) & (lane < 16 * i + 8), mine, 0.0)
    gram_ref[...] = out


def finish_kernel(table_ref, sums_ref, own_ref, v_ref, corr_ref, new_ref, est_ref):
    moments = sums_ref[0]
    for k in range(1, sums_ref.shape[0]):
        moments += sums_ref[k]
    lane = lax.broadcasted_iota(jnp.int32, (NRHS, LANES), 1)
    row = lax.broadcasted_iota(jnp.int32, (NRHS, LANES), 0)
    rolled = [moments if d == 0 else pltpu.roll(moments, (8 * d) % LANES, 1) for d in ROLLS]
    m = []
    for i in range(DEPTH):
        total = jnp.zeros((NRHS, LANES), jnp.float32)
        for k in range(len(ROLLS)):
            total += table_ref[i * len(ROLLS) + k : i * len(ROLLS) + k + 1, :] * rolled[k]
        m.append(total)
    right = list(m)
    for k in range(DEPTH * NRHS):
        i, r = divmod(k, NRHS)
        cols = [jnp.broadcast_to(m[j][:, k : k + 1], (NRHS, LANES)) for j in range(DEPTH)]
        pivot = jnp.broadcast_to(cols[i][r : r + 1, :], (NRHS, LANES))
        line = jnp.broadcast_to(m[i][r : r + 1, :], (NRHS, LANES)) / pivot
        m = [m[j] - cols[j] * line for j in range(DEPTH)]
        m[i] = jnp.where(row == r, line, m[i])
    first = (lane >= 8 * DEPTH) & (lane < 8 * DEPTH + 8)
    c = [jnp.where(first, m[j], 0.0) for j in range(DEPTH)]
    initial = jnp.sum(jnp.where(row == lane, moments, 0.0), 0, keepdims=True)
    initial = pltpu.roll(jnp.broadcast_to(initial, (NRHS, LANES)), 8 * DEPTH, 1)
    gain = right[0] * c[0]
    for j in range(1, DEPTH):
        gain += right[j] * c[j]
    gain = jnp.sum(gain, 0, keepdims=True)
    est = (initial - gain) / initial
    est_ref[...] = est[:1, 8 * DEPTH : 8 * DEPTH + 8]
    rows = []
    for j in range(DEPTH + 1):
        w = jnp.zeros((NRHS, LANES), jnp.float32)
        if j < DEPTH:
            w += SHIFTS[j] * c[j]
        if j:
            w += SCALE_POWER * c[j - 1]
        kept = -pltpu.roll(w, LANES - 24, 1)
        if j == 0:
            kept = jnp.where(lane == row + 8, 1.0, 0.0) + kept
        if j < DEPTH:
            kept = jnp.where(lane < 8, pltpu.roll(c[j], LANES - 32, 1), kept)
        rows.append(kept)
    rows.append(jnp.zeros((LANES - len(rows) * NRHS, LANES), jnp.float32))
    mix = jnp.transpose(jnp.concatenate(rows, 0))[:16, : (DEPTH + 1) * NRHS]
    for x in range(CX):
        parts = []
        for y in range(CY):
            stack = [own_ref[x * CY + y]]
            stack += [v_ref[j, x * WY + DEPTH + y] for j in range(DEPTH)]
            parts.append(
                jnp.dot(
                    mix,
                    jnp.concatenate(stack, 0),
                    precision=HIGHEST,
                    preferred_element_type=jnp.float32,
                )
            )
        both = jnp.stack(parts, 0)
        corr_ref[:, x] = jnp.swapaxes(both[:, :8], 0, 1)
        new_ref[:, x] = jnp.swapaxes(both[:, 8:], 0, 1)


VMEM = pl.BlockSpec(memory_space=pltpu.VMEM)
SMEM = pl.BlockSpec(memory_space=pltpu.SMEM)


def f32(*shape):
    return jax.ShapeDtypeStruct(shape, jnp.float32)


def call(kernel, specs, out_shape, *args, scratch=(), limit=12, flops=10**8):
    return pl.pallas_call(
        kernel,
        in_specs=specs,
        out_specs=jax.tree.map(lambda _: VMEM, out_shape),
        out_shape=out_shape,
        scratch_shapes=scratch,
        cost_estimate=pl.CostEstimate(flops=flops, bytes_accessed=10**6, transcendentals=0),
        compiler_params=pltpu.CompilerParams(vmem_limit_bytes=limit * 2**20),
    )(*args)


def swaps(count, odd):
    out = []
    for i in range(odd, count - 1, 2):
        out += [(i, i + 1), (i + 1, i)]
    return out


def spread(x, axes):
    count = lax.axis_size(axes)
    return lax.all_to_all(jnp.broadcast_to(x[None], (count, *x.shape)), axes, 0, 0, tiled=True)


def body(residual_block, diagonal):
    at_x, at_y = lax.axis_index(GX), lax.axis_index("gy")
    count_x, count_y = lax.axis_size(GX), lax.axis_size("gy")
    par = jnp.stack(
        [
            at_x % 2,
            at_y % 2,
            at_x == 0,
            at_x == count_x - 1,
            at_y == 0,
            at_y == count_y - 1,
        ]
    ).astype(jnp.int32)
    own = call(pack_kernel, [VMEM] * 2, f32(PACK, NRHS, CZ), residual_block, diagonal)
    odd = lax.ppermute(own, GX, swaps(count_x, 1))
    even = lax.ppermute(own, GX, swaps(count_x, 0))
    die, link = call(
        side_kernel, [SMEM] + [VMEM] * 3, [f32(SIDE_PACK, NRHS, CZ)] * 2, par, own, even, odd
    )
    link = lax.ppermute(link, "gy", swaps(count_y, 1))
    die = lax.ppermute(die, "gy", swaps(count_y, 0))
    v, gram = call(
        basis_kernel,
        [SMEM] + [VMEM] * 5,
        [f32(DEPTH, CX * WY, NRHS, CZ), f32(NRHS, LANES)],
        par,
        own,
        even,
        odd,
        die,
        link,
        scratch=[pltpu.VMEM((WX * WY, NRHS, CZ), jnp.float32)] * DEPTH
        + [
            pltpu.VMEM((WX, WY, CZ), jnp.float32),
            pltpu.VMEM((WX * WY, NRHS, CZ), jnp.float32),
        ],
        limit=16,
    )
    sums = spread(spread(gram, NEAR).sum(0), FAR)
    corr, new, est = call(
        finish_kernel,
        [VMEM] * 4,
        [f32(*residual_block.shape), f32(*residual_block.shape), f32(1, NRHS)],
        jnp.asarray(roll_table()),
        sums,
        own,
        v,
    )
    return corr, new, est.reshape(NRHS)


def solution(mesh):
    split = Mesh(mesh.devices.reshape(16, 2, 4, mesh.shape["gy"]), ("z1", "z0", "y", "gy"))
    return jax.shard_map(
        body,
        mesh=split,
        in_specs=(P(None, GX, "gy", None), P(GX, "gy", None)),
        out_specs=(P(None, GX, "gy", None), P(None, GX, "gy", None), P()),
        check_vma=False,
    )
```

```python
import jax
import jax.numpy as jnp
import numpy as np
from jax import lax
from jax.experimental import pallas as pl
from jax.experimental.pallas import tpu as pltpu
from jax.sharding import Mesh
from jax.sharding import PartitionSpec as P

NRHS = 8
WEIGHT_X = 0.4
WEIGHT_Y = 0.2
WEIGHT_Z = 0.1
CENTRE = 2.2
SCALE_POWER = 3.0
THIRD = 1.0 / SCALE_POWER
SHIFTS = (6.0, 1.5, 4.5, 3.0)
DEPTH = len(SHIFTS)

CX, CY, CZ = 4, 8, 256
WX, WY = CX + 2 * DEPTH, CY + 2 * DEPTH
LANES = 128

GX = ("z1", "z0", "y")
NEAR = ("z0", "y", "gy")
FAR = ("z1",)
OWN = CX * CY
PACK = OWN + CX
NEXT = CX * DEPTH + CX // 2
REST = 2 * CX * DEPTH + CX
BLOCKS = 2 * DEPTH + 1
USED = BLOCKS * NRHS
MESSAGE = 3 * LANES


def moment_terms():
    table = {}
    for j in range(DEPTH + 1):
        for i in (j, j + 1):
            if i <= DEPTH:
                table[i, j] = np.eye(BLOCKS)[2 * j + (i - j)]
    for gap in range(2, DEPTH + 1):
        for j in range(DEPTH + 1 - gap):
            i = j + gap - 1
            low = table[i, j + 1]
            table[i + 1, j] = low + (SHIFTS[j] - SHIFTS[i]) / SCALE_POWER * table[i, j]

    def block(i, j):
        return table[max(i, j), min(i, j)]

    alpha = np.zeros((BLOCKS, DEPTH, DEPTH + 1))
    for i in range(DEPTH):
        for j in range(DEPTH):
            alpha[:, i, j] = (
                SHIFTS[i] * SHIFTS[j] * block(i, j)
                + SCALE_POWER * SHIFTS[i] * block(i, j + 1)
                + SCALE_POWER * SHIFTS[j] * block(i + 1, j)
                + SCALE_POWER**2 * block(i + 1, j + 1)
            )
        alpha[:, i, DEPTH] = SHIFTS[i] * block(i, 0) + SCALE_POWER * block(i + 1, 0)
    return alpha


ROLLS = range(1 - BLOCKS, DEPTH)


def roll_table():
    alpha = moment_terms()
    out = np.zeros(((DEPTH + 1) * len(ROLLS), LANES), np.float32)
    for j in range(DEPTH + 1):
        for k, d in enumerate(ROLLS):
            for i in range(DEPTH):
                if 0 <= i - d < BLOCKS:
                    out[j * len(ROLLS) + k, 8 * i : 8 * i + 8] = alpha[i - d, i, j]
    return out


def iota(axis):
    return lax.broadcasted_iota(jnp.int32, (NRHS, LANES), axis)


def spin(x, by):
    by %= LANES
    return pltpu.roll(x, by, 1) if by else x


def halves(a, b, first):
    low = lax.broadcasted_iota(jnp.int32, (CY, CZ), 0) < DEPTH
    if first:
        return jnp.where(low, pltpu.roll(a, DEPTH, 0), b)
    return jnp.where(low, a, pltpu.roll(b, DEPTH, 0))


def pack_kernel(par_ref, res_hbm, diag_hbm, out_ref, next_ref, res_ref, diag_ref, sems):
    core = par_ref[1]
    copies = (
        pltpu.make_async_copy(res_hbm, res_ref, sems.at[0]),
        pltpu.make_async_copy(diag_hbm, diag_ref, sems.at[1]),
    )
    for copy in copies:
        copy.start()
    for copy in copies:
        copy.wait()
    for x in range(CX):
        out_ref[CY * x : CY * x + CY] = jnp.swapaxes(res_ref[:, x], 0, 1)
        out_ref[OWN + x] = diag_ref[x]
    first = DEPTH * core
    for x in range(CX):
        for k in range(DEPTH):
            next_ref[DEPTH * x + k] = out_ref[CY * x + first + k]
    for k in range(CX // 2):
        a, b = diag_ref[2 * k], diag_ref[2 * k + 1]
        next_ref[CX * DEPTH + k] = jnp.where(core == 0, halves(a, b, 0), halves(a, b, DEPTH))


def side_kernel(par_ref, own_ref, even_ref, odd_ref, next_ref, die_ref, link_ref):
    del next_ref
    px, core = par_ref[0], par_ref[1]
    sides = ((own_ref, CX), (even_ref, 2 * CX * (1 - px)), (odd_ref, 2 * CX * px))
    for which, (ref, base) in enumerate(sides):
        packed = base // 2 if which else 0
        for x in range(CX):
            for k in range(DEPTH):
                die_ref[(base + x) * DEPTH + k] = ref[CY * x + DEPTH * (1 - core) + k]
                if which:
                    link_ref[(packed + x) * DEPTH + k] = ref[CY * x + DEPTH * core + k]
        for k in range(CX // 2):
            a, b = ref[OWN + 2 * k], ref[OWN + 2 * k + 1]
            low, high = halves(a, b, 0), halves(a, b, DEPTH)
            die_ref[WX * DEPTH + base // 2 + k] = jnp.where(core == 0, high, low)
            if which:
                link_ref[2 * CX * DEPTH + packed // 2 + k] = jnp.where(core == 0, low, high)


def place(e_ref, v_ref, level, x):
    if level and DEPTH <= x < DEPTH + CX:
        return v_ref.at[level - 1], (x - DEPTH) * WY
    return e_ref.at[level], x * WY


def advance(e_ref, v_ref, bc_ref, level, rows):
    margin = level + 1
    lane = iota(1)
    for y in rows:
        centre, total = {}, {}
        for x in range(level, WX - level):
            ref, at = place(e_ref, v_ref, level, x)
            centre[x] = ref[at + y]
            total[x] = centre[x] + WEIGHT_Y * (ref[at + y - 1] + ref[at + y + 1])
        for x in range(margin, WX - margin):
            t = total[x] + WEIGHT_X * (total[x - 1] + total[x + 1])
            a, b = t[:, :LANES], t[:, LANES:]
            up_a, up_b = spin(a, 1), spin(b, 1)
            dn_a, dn_b = spin(a, -1), spin(b, -1)
            near_a = jnp.where(lane == 0, 0.0, up_a) + jnp.where(lane == LANES - 1, dn_b, dn_a)
            near_b = jnp.where(lane == 0, up_a, up_b) + jnp.where(lane == LANES - 1, 0.0, dn_b)
            coeff = bc_ref[x * WY + y] - SHIFTS[level] * THIRD
            ref, at = place(e_ref, v_ref, level + 1, x)
            ref[at + y, :, :LANES] = coeff[:, :LANES] * centre[x][:, :LANES] - THIRD * (
                a + WEIGHT_Z * near_a
            )
            ref[at + y, :, LANES:] = coeff[:, LANES:] * centre[x][:, LANES:] - THIRD * (
                b + WEIGHT_Z * near_b
            )


def clear(e_ref, v_ref, level, xs, ys):
    zero = jnp.zeros((NRHS, CZ), jnp.float32)

    @pl.loop(ys[0], ys[1])
    def _(y):
        for x in range(*xs):
            ref, at = place(e_ref, v_ref, level, x)
            ref[at + y] = zero


def clear_planes(par_ref, e_ref, v_ref, level, spans):
    for index, xs in ((2, (level, DEPTH)), (3, (DEPTH + CX, WX - level))):

        @pl.when(par_ref[index] == 1)
        def _(xs=xs):
            for ys in spans:
                clear(e_ref, v_ref, level, xs, ys)


def scaled(line):
    return jnp.broadcast_to((line + (CENTRE + 1.0)) * THIRD, (NRHS, CZ))


def inner_kernel(par_ref, own_ref, even_ref, odd_ref, e_ref, v_ref, bc_ref):
    px = par_ref[0]
    for ref, base in ((own_ref, CX), (even_ref, 2 * CX * (1 - px)), (odd_ref, 2 * CX * px)):
        for x in range(CX):
            for y in range(CY):
                at = (base + x) * WY + DEPTH + y
                e_ref[0, at] = ref[CY * x + y]
                bc_ref[at] = scaled(ref[OWN + x, y : y + 1])
    for level in range(DEPTH - 1):
        low, high = DEPTH + level + 1, DEPTH + CY - level - 1
        advance(e_ref, v_ref, bc_ref, level, range(low, high))
        clear_planes(par_ref, e_ref, v_ref, level + 1, ((low, high),))


def split(a):
    high = a.astype(jnp.bfloat16).astype(jnp.float32)
    rest = a - high
    middle = rest.astype(jnp.bfloat16).astype(jnp.float32)
    return high, middle, rest - middle


def basis_kernel(
    par_ref, own_ref, next_ref, link_ref, die_ref, e_in, v_in, bc_in, e_ref, v_ref, bc_ref, out_ref
):
    del e_in, v_in, bc_in
    core = par_ref[1]
    die_at, link_at = 3 * DEPTH * (1 - core), 3 * DEPTH * core
    sources = [(die_ref, x, x, WX, die_at) for x in range(WX)]
    sources += [(next_ref, x, CX + x, CX, link_at) for x in range(CX)]
    sources += [(link_ref, x, x if x < CX else CX + x, 2 * CX, link_at) for x in range(2 * CX)]
    for ref, mine, x, count, base in sources:
        for k in range(DEPTH):
            at = x * WY + base + k
            e_ref[0, at] = ref[mine * DEPTH + k]
            row = DEPTH * (mine % 2) + k
            bc_ref[at] = scaled(ref[count * DEPTH + mine // 2, row : row + 1])
    for level in range(DEPTH):
        m = level + 1
        low, high = DEPTH + m, DEPTH + CY - m
        if low >= high:
            rows = (range(m, WY - m),)
        else:
            rows = (range(m, low), range(high, WY - m))
        for part in rows:
            advance(e_ref, v_ref, bc_ref, level, part)
        if m < DEPTH:
            clear_planes(par_ref, e_ref, v_ref, m, [(part[0], part[-1] + 1) for part in rows])
            for index, ys in ((4, (m, DEPTH)), (5, (DEPTH + CY, WY - m))):

                @pl.when(par_ref[index] == 1)
                def _(ys=ys, m=m):
                    clear(e_ref, v_ref, m, (m, WX - m), ys)

    def add(x, total):
        for y in range(CY):
            parts = [split(own_ref[x * CY + y])]
            parts += [split(v_ref[j, x * WY + DEPTH + y]) for j in range(DEPTH)]
            stack = [part[k] for k in range(3) for part in parts]
            stack.append(jnp.zeros((NRHS, CZ), jnp.float32))
            w = jnp.concatenate(stack, 0).astype(jnp.bfloat16)
            total += lax.dot_general(
                w, w, (((1,), (1,)), ((), ())), preferred_element_type=jnp.float32
            )
        return total

    gram = lax.fori_loop(0, CX, add, jnp.zeros((LANES, LANES), jnp.float32))
    lane, row = iota(1), iota(0)
    moments = jnp.zeros((NRHS, LANES), jnp.float32)
    count = (DEPTH + 1) * NRHS
    for i in range(DEPTH + 1):
        mine = sum(gram[k * count + 8 * i : k * count + 8 * i + 8] for k in range(3))
        mine = spin(mine, 8 * i) + spin(mine, 8 * i - count) + spin(mine, 8 * i - 2 * count)
        moments += jnp.where((lane >= 16 * i - 8) & (lane < 16 * i + 8), mine, 0.0)
    turn = [
        jnp.sum(jnp.where(row == ((lane - k) & 7), moments, 0.0), 0, keepdims=True)
        for k in range(5)
    ]
    at = lane[:1]
    out_ref[:, :LANES] = jnp.where(at < USED, turn[0], spin(turn[3], USED))
    out_ref[:, LANES : 2 * LANES] = jnp.where(
        at < USED, turn[1], jnp.where(at < 88, spin(turn[3], 16), spin(turn[4], 88))
    )
    out_ref[:, 2 * LANES :] = jnp.where(at < USED, turn[2], spin(turn[4], 32))


def unpack(sums):
    at, lane, row = iota(1)[:1], iota(1), iota(0)
    a, b, c = sums[:, :LANES], sums[:, LANES : 2 * LANES], sums[:, 2 * LANES :]
    turn = [a, b, c]
    turn.append(jnp.where(at < 56, spin(a, 56), spin(b, -16)))
    turn.append(jnp.where(at < 40, spin(b, 40), spin(c, -32)))
    for k in (5, 6, 7):
        j = 8 - k
        turn.append(jnp.where((at & 7) + j < 8, spin(turn[j], -j), spin(turn[j], 8 - j)))
    moments = jnp.zeros((NRHS, LANES), jnp.float32)
    for k in range(8):
        moments += jnp.where(
            (((lane - row) & 7) == k) & (lane < USED),
            jnp.broadcast_to(turn[k], (NRHS, LANES)),
            0.0,
        )
    return moments


def solve(table_ref, moments):
    lane = iota(1)
    rolled = [spin(moments, 8 * d) for d in ROLLS]
    a = []
    for j in range(DEPTH + 1):
        total = jnp.zeros((NRHS, LANES), jnp.float32)
        for k in range(len(ROLLS)):
            at = j * len(ROLLS) + k
            total += table_ref[at : at + 1, :] * rolled[k]
        a.append(total)
    right = a[DEPTH]
    for q in range(DEPTH):
        live = range(q, DEPTH + 1)
        col = [
            {j: jnp.broadcast_to(a[j][:, 8 * q + c : 8 * q + c + 1], (NRHS, LANES)) for j in live}
            for c in range(NRHS)
        ]
        for c in range(NRHS):
            k = 8 * q + c
            inverse = 1.0 / jnp.broadcast_to(col[c][q][c : c + 1], (NRHS, LANES))
            line = jnp.broadcast_to(a[q][c : c + 1], (NRHS, LANES)) * inverse
            for j in live:
                a[j] = jnp.where(lane == k, col[c][j] * inverse, a[j] - col[c][j] * line)
            for d in range(c + 1, NRHS):
                factor = jnp.broadcast_to(col[d][q][c : c + 1], (NRHS, LANES)) * inverse
                for j in live:
                    col[d][j] = col[d][j] - col[c][j] * factor
    return jnp.where(lane < DEPTH * NRHS, a[DEPTH], 0.0), right


def finish_kernel(table_ref, sums_ref, own_ref, v_ref, corr_ref, new_ref, est_ref):
    sums = sums_ref[0]
    for k in range(1, sums_ref.shape[0]):
        sums += sums_ref[k]
    moments = unpack(sums)
    lane, row = iota(1), iota(0)
    coeffs, right = solve(table_ref, moments)
    initial = jnp.sum(jnp.where(lane == row, moments, 0.0), 1, keepdims=True)
    gain = jnp.sum(right * coeffs, 1, keepdims=True)
    est = jnp.broadcast_to((initial - gain) / initial, (NRHS, LANES))
    est = jnp.sum(jnp.where(lane == row, est, 0.0), 0, keepdims=True)
    est_ref[...] = est[:, :NRHS]
    shift = jnp.zeros((NRHS, LANES), jnp.float32)
    for j in range(DEPTH):
        shift = jnp.where((lane >= 8 * j) & (lane < 8 * j + 8), SHIFTS[j], shift)
    kept = jnp.where(lane == row, 1.0, 0.0) - (shift * coeffs + SCALE_POWER * spin(coeffs, 8))
    high, middle, low = split(jnp.concatenate([coeffs, kept], 0))
    lane = lax.broadcasted_iota(jnp.int32, (2 * NRHS, LANES), 1)
    count = (DEPTH + 1) * NRHS
    middle_at = spin(middle, 3 * count)
    first = high + spin(high, count) + spin(high, 2 * count)
    first += jnp.where(lane >= 3 * count, middle_at, 0.0)
    second = jnp.where(lane < 4 * count - LANES, middle_at, 0.0)
    second += spin(middle, 4 * count) + spin(low, 5 * count)
    mix = jnp.concatenate([first, second], 1).astype(jnp.bfloat16)
    for x in range(CX):
        parts = []
        for y in range(CY):
            terms = [split(own_ref[x * CY + y])]
            terms += [split(v_ref[j, x * WY + DEPTH + y]) for j in range(DEPTH)]
            stack = [term[k] for k in (0, 1, 2, 0, 1, 0) for term in terms]
            stack += [jnp.zeros((NRHS, CZ), jnp.float32)] * 2
            w = jnp.concatenate(stack, 0).astype(jnp.bfloat16)
            parts.append(jnp.dot(mix, w, preferred_element_type=jnp.float32))
        both = jnp.stack(parts, 0)
        corr_ref[:, x] = jnp.swapaxes(both[:, :NRHS], 0, 1)
        new_ref[:, x] = jnp.swapaxes(both[:, NRHS:], 0, 1)


VMEM = pl.BlockSpec(memory_space=pltpu.VMEM)
SMEM = pl.BlockSpec(memory_space=pltpu.SMEM)
HBM = pl.BlockSpec(memory_space=pltpu.HBM)


def f32(*shape):
    return jax.ShapeDtypeStruct(shape, jnp.float32)


def call(kernel, specs, out_shape, *args, scratch=(), limit=12, flops=10**8, aliases=None):
    return pl.pallas_call(
        kernel,
        in_specs=specs,
        out_specs=jax.tree.map(lambda _: VMEM, out_shape),
        out_shape=out_shape,
        scratch_shapes=scratch,
        input_output_aliases=aliases or {},
        cost_estimate=pl.CostEstimate(flops=flops, bytes_accessed=10**6, transcendentals=0),
        compiler_params=pltpu.CompilerParams(vmem_limit_bytes=limit * 2**20),
    )(*args)


def swaps(count, odd):
    out = []
    for i in range(odd, count - 1, 2):
        out += [(i, i + 1), (i + 1, i)]
    return out


def spread(x, axes, groups=None):
    count = lax.axis_size(axes)
    copies = jnp.broadcast_to(x[None], (count, *x.shape))
    return lax.all_to_all(copies, axes, 0, 0, tiled=True, axis_index_groups=groups)


def body(residual_block, diagonal):
    at_x, at_y = lax.axis_index(GX), lax.axis_index("gy")
    count_x, count_y = lax.axis_size(GX), lax.axis_size("gy")
    par = jnp.stack(
        [
            at_x & 1,
            at_y & 1,
            at_x == 0,
            at_x == count_x - 1,
            at_y == 0,
            at_y == count_y - 1,
        ]
    ).astype(jnp.int32)
    own, nxt = call(
        pack_kernel,
        [SMEM, HBM, HBM],
        [f32(PACK, NRHS, CZ), f32(NEXT, NRHS, CZ)],
        par,
        residual_block,
        diagonal,
        scratch=[
            pltpu.VMEM(residual_block.shape, jnp.float32),
            pltpu.VMEM(diagonal.shape, jnp.float32),
            pltpu.SemaphoreType.DMA((2,)),
        ],
    )
    odd = lax.ppermute(own, GX, swaps(count_x, 1))
    even = lax.ppermute(own, GX, swaps(count_x, 0))
    nxt = lax.ppermute(nxt, "gy", swaps(count_y, 1))
    die, link = call(
        side_kernel,
        [SMEM] + [VMEM] * 4,
        [f32(WX * DEPTH + WX // 2, NRHS, CZ), f32(REST, NRHS, CZ)],
        par,
        own,
        even,
        odd,
        nxt,
    )
    link = lax.ppermute(link, "gy", swaps(count_y, 1))
    die = lax.ppermute(die, "gy", swaps(count_y, 0))
    state = [
        f32(DEPTH, WX * WY, NRHS, CZ),
        f32(DEPTH, CX * WY, NRHS, CZ),
        f32(WX * WY, NRHS, CZ),
    ]
    e, v, bc = call(inner_kernel, [SMEM] + [VMEM] * 3, state, par, own, even, odd)
    e, v, bc, message = call(
        basis_kernel,
        [SMEM] + [VMEM] * 7,
        [*state, f32(1, MESSAGE)],
        par,
        own,
        nxt,
        link,
        die,
        e,
        v,
        bc,
        aliases={5: 0, 6: 1, 7: 2},
    )
    count = lax.axis_size(FAR)
    order = [[(count // 2 + i) % count for i in range(count)]]
    sums = spread(spread(message, NEAR).sum(0), FAR, order)
    corr, new, est = call(
        finish_kernel,
        [VMEM] * 4,
        [f32(*residual_block.shape), f32(*residual_block.shape), f32(1, NRHS)],
        jnp.asarray(roll_table()),
        sums,
        own,
        v,
    )
    return corr, new, est.reshape(NRHS)


def solution(mesh):
    split_mesh = Mesh(mesh.devices.reshape(16, 2, 4, mesh.shape["gy"]), ("z1", "z0", "y", "gy"))
    return jax.shard_map(
        body,
        mesh=split_mesh,
        in_specs=(P(None, GX, "gy", None), P(GX, "gy", None)),
        out_specs=(P(None, GX, "gy", None), P(None, GX, "gy", None), P()),
        check_vma=False,
    )
```

```python
import jax
import jax.numpy as jnp
import numpy as np
from jax import lax
from jax.experimental import pallas as pl
from jax.experimental.pallas import tpu as pltpu
from jax.sharding import Mesh
from jax.sharding import PartitionSpec as P

NRHS = 8
WEIGHT_X = 0.4
WEIGHT_Y = 0.2
WEIGHT_Z = 0.1
CENTRE = 2.2
SCALE_POWER = 3.0
THIRD = 1.0 / SCALE_POWER
SHIFTS = (6.0, 1.5, 4.5, 3.0)
DEPTH = len(SHIFTS)

CX, CY, CZ = 4, 8, 256
WX, WY = CX + 2 * DEPTH, CY + 2 * DEPTH
LANES = 128

GX = ("z1", "z0", "y")
NEAR = ("z0", "y", "gy")
FAR = ("z1",)
OWN = CX * CY
PACK = OWN + CX
NEXT = CX * DEPTH + CX // 2
REST = 2 * CX * DEPTH + CX
BLOCKS = 2 * DEPTH + 1
USED = BLOCKS * NRHS
MESSAGE = 3 * LANES


def moment_terms():
    table = {}
    for j in range(DEPTH + 1):
        for i in (j, j + 1):
            if i <= DEPTH:
                table[i, j] = np.eye(BLOCKS)[2 * j + (i - j)]
    for gap in range(2, DEPTH + 1):
        for j in range(DEPTH + 1 - gap):
            i = j + gap - 1
            low = table[i, j + 1]
            table[i + 1, j] = low + (SHIFTS[j] - SHIFTS[i]) / SCALE_POWER * table[i, j]

    def block(i, j):
        return table[max(i, j), min(i, j)]

    alpha = np.zeros((BLOCKS, DEPTH, DEPTH + 1))
    for i in range(DEPTH):
        for j in range(DEPTH):
            alpha[:, i, j] = (
                SHIFTS[i] * SHIFTS[j] * block(i, j)
                + SCALE_POWER * SHIFTS[i] * block(i, j + 1)
                + SCALE_POWER * SHIFTS[j] * block(i + 1, j)
                + SCALE_POWER**2 * block(i + 1, j + 1)
            )
        alpha[:, i, DEPTH] = SHIFTS[i] * block(i, 0) + SCALE_POWER * block(i + 1, 0)
    return alpha


ROLLS = range(1 - BLOCKS, DEPTH)


def roll_table():
    alpha = moment_terms()
    out = np.zeros(((DEPTH + 1) * len(ROLLS), LANES), np.float32)
    for j in range(DEPTH + 1):
        for k, d in enumerate(ROLLS):
            for i in range(DEPTH):
                if 0 <= i - d < BLOCKS:
                    out[j * len(ROLLS) + k, 8 * i : 8 * i + 8] = alpha[i - d, i, j]
    return out


def iota(axis):
    return lax.broadcasted_iota(jnp.int32, (NRHS, LANES), axis)


def spin(x, by):
    by %= LANES
    return pltpu.roll(x, by, 1) if by else x


def halves(a, b, first):
    low = lax.broadcasted_iota(jnp.int32, (CY, CZ), 0) < DEPTH
    if first:
        return jnp.where(low, pltpu.roll(a, DEPTH, 0), b)
    return jnp.where(low, a, pltpu.roll(b, DEPTH, 0))


def pack(raw_ref, ref):
    for x in range(CX):
        ref[CY * x : CY * x + CY] = jnp.swapaxes(raw_ref[:NRHS, x], 0, 1)
        ref[OWN + x] = raw_ref[NRHS, x]


def rows_of(ref, base, count, up_ref, down_ref):
    for out_ref, first in ((up_ref, CY - DEPTH), (down_ref, 0)):
        for x in range(CX):
            for k in range(DEPTH):
                out_ref[(base + x) * DEPTH + k] = ref[CY * x + first + k]
        for k in range(CX // 2):
            pair = halves(ref[OWN + 2 * k], ref[OWN + 2 * k + 1], first)
            out_ref[count * DEPTH + base // 2 + k] = pair


def pack_kernel(raw_ref, out_ref, up_ref, down_ref):
    pack(raw_ref, out_ref)
    rows_of(out_ref, 0, CX, up_ref, down_ref)


def side_kernel(evens_ref, odds_ref, up_ref, down_ref, even_ref, odd_ref):
    px = lax.axis_index("y") & 1
    pack(evens_ref, even_ref)
    pack(odds_ref, odd_ref)
    rows_of(even_ref, CX * (1 - px), 2 * CX, up_ref, down_ref)
    rows_of(odd_ref, CX * px, 2 * CX, up_ref, down_ref)


def place(e_ref, v_ref, level, x):
    if level and DEPTH <= x < DEPTH + CX:
        return v_ref.at[level - 1], (x - DEPTH) * WY
    return e_ref.at[level], x * WY


def advance(e_ref, v_ref, bc_ref, level, rows):
    margin = level + 1
    lane = iota(1)
    for y in rows:
        centre, total = {}, {}
        for x in range(level, WX - level):
            ref, at = place(e_ref, v_ref, level, x)
            centre[x] = ref[at + y]
            total[x] = centre[x] + WEIGHT_Y * (ref[at + y - 1] + ref[at + y + 1])
        for x in range(margin, WX - margin):
            t = total[x] + WEIGHT_X * (total[x - 1] + total[x + 1])
            a, b = t[:, :LANES], t[:, LANES:]
            up_a, up_b = spin(a, 1), spin(b, 1)
            dn_a, dn_b = spin(a, -1), spin(b, -1)
            near_a = jnp.where(lane == 0, 0.0, up_a) + jnp.where(lane == LANES - 1, dn_b, dn_a)
            near_b = jnp.where(lane == 0, up_a, up_b) + jnp.where(lane == LANES - 1, 0.0, dn_b)
            coeff = bc_ref[x * WY + y] - SHIFTS[level] * THIRD
            ref, at = place(e_ref, v_ref, level + 1, x)
            ref[at + y, :, :LANES] = coeff[:, :LANES] * centre[x][:, :LANES] - THIRD * (
                a + WEIGHT_Z * near_a
            )
            ref[at + y, :, LANES:] = coeff[:, LANES:] * centre[x][:, LANES:] - THIRD * (
                b + WEIGHT_Z * near_b
            )


def clear(e_ref, v_ref, level, xs, ys):
    zero = jnp.zeros((NRHS, CZ), jnp.float32)

    @pl.loop(ys[0], ys[1])
    def _(y):
        for x in range(*xs):
            ref, at = place(e_ref, v_ref, level, x)
            ref[at + y] = zero


def clear_planes(e_ref, v_ref, level, spans):
    at, last = lax.axis_index(GX), lax.axis_size(GX) - 1
    for edge, xs in ((0, (level, DEPTH)), (last, (DEPTH + CX, WX - level))):

        @pl.when(at == edge)
        def _(xs=xs):
            for ys in spans:
                clear(e_ref, v_ref, level, xs, ys)


def scaled(line):
    return jnp.broadcast_to((line + (CENTRE + 1.0)) * THIRD, (NRHS, CZ))


def inner_kernel(own_ref, even_ref, odd_ref, e_ref, v_ref, bc_ref):
    px = lax.axis_index("y") & 1
    for ref, base in ((own_ref, CX), (even_ref, 2 * CX * (1 - px)), (odd_ref, 2 * CX * px)):
        for x in range(CX):
            for y in range(CY):
                at = (base + x) * WY + DEPTH + y
                e_ref[0, at] = ref[CY * x + y]
                bc_ref[at] = scaled(ref[OWN + x, y : y + 1])
    for level in range(DEPTH - 1):
        low, high = DEPTH + level + 1, DEPTH + CY - level - 1
        advance(e_ref, v_ref, bc_ref, level, range(low, high))
        clear_planes(e_ref, v_ref, level + 1, ((low, high),))


def split(a):
    high = a.astype(jnp.bfloat16).astype(jnp.float32)
    rest = a - high
    middle = rest.astype(jnp.bfloat16).astype(jnp.float32)
    return high, middle, rest - middle


def basis_kernel(
    own_ref, lows, highs, e_in, v_in, bc_in, e_ref, v_ref, bc_ref, out_ref
):
    del e_in, v_in, bc_in
    at_y, last_y = lax.axis_index("gy"), lax.axis_size("gy") - 1
    for (near_ref, rest_ref), base, edge in ((lows, 0, 0), (highs, DEPTH + CY, last_y)):
        sources = [(near_ref, x, CX + x, CX) for x in range(CX)]
        sources += [(rest_ref, x, x if x < CX else CX + x, 2 * CX) for x in range(2 * CX)]
        for ref, mine, x, count in sources:
            for k in range(DEPTH):
                at = x * WY + base + k
                e_ref[0, at] = ref[mine * DEPTH + k]
                row = DEPTH * (mine % 2) + k
                bc_ref[at] = scaled(ref[count * DEPTH + mine // 2, row : row + 1])

        @pl.when(at_y == edge)
        def _(base=base):
            clear(e_ref, v_ref, 0, (0, WX), (base, base + DEPTH))

    for level in range(DEPTH):
        m = level + 1
        low, high = DEPTH + m, DEPTH + CY - m
        if low >= high:
            rows = (range(m, WY - m),)
        else:
            rows = (range(m, low), range(high, WY - m))
        for part in rows:
            advance(e_ref, v_ref, bc_ref, level, part)
        if m < DEPTH:
            clear_planes(e_ref, v_ref, m, [(part[0], part[-1] + 1) for part in rows])
            for edge, ys in ((0, (m, DEPTH)), (last_y, (DEPTH + CY, WY - m))):

                @pl.when(at_y == edge)
                def _(ys=ys, m=m):
                    clear(e_ref, v_ref, m, (m, WX - m), ys)

    def add(x, total):
        for y in range(CY):
            parts = [split(own_ref[x * CY + y])]
            parts += [split(v_ref[j, x * WY + DEPTH + y]) for j in range(DEPTH)]
            stack = [part[k] for k in range(3) for part in parts]
            stack.append(jnp.zeros((NRHS, CZ), jnp.float32))
            w = jnp.concatenate(stack, 0).astype(jnp.bfloat16)
            total += lax.dot_general(
                w, w, (((1,), (1,)), ((), ())), preferred_element_type=jnp.float32
            )
        return total

    gram = lax.fori_loop(0, CX, add, jnp.zeros((LANES, LANES), jnp.float32))
    lane, row = iota(1), iota(0)
    moments = jnp.zeros((NRHS, LANES), jnp.float32)
    count = (DEPTH + 1) * NRHS
    for i in range(DEPTH + 1):
        mine = sum(gram[k * count + 8 * i : k * count + 8 * i + 8] for k in range(3))
        mine = spin(mine, 8 * i) + spin(mine, 8 * i - count) + spin(mine, 8 * i - 2 * count)
        moments += jnp.where((lane >= 16 * i - 8) & (lane < 16 * i + 8), mine, 0.0)
    turn = [
        jnp.sum(jnp.where(row == ((lane - k) & 7), moments, 0.0), 0, keepdims=True)
        for k in range(5)
    ]
    at = lane[:1]
    out_ref[:, :LANES] = jnp.where(at < USED, turn[0], spin(turn[3], USED))
    out_ref[:, LANES : 2 * LANES] = jnp.where(
        at < USED, turn[1], jnp.where(at < 88, spin(turn[3], 16), spin(turn[4], 88))
    )
    out_ref[:, 2 * LANES :] = jnp.where(at < USED, turn[2], spin(turn[4], 32))


def unpack(sums):
    at, lane, row = iota(1)[:1], iota(1), iota(0)
    a, b, c = sums[:, :LANES], sums[:, LANES : 2 * LANES], sums[:, 2 * LANES :]
    turn = [a, b, c]
    turn.append(jnp.where(at < 56, spin(a, 56), spin(b, -16)))
    turn.append(jnp.where(at < 40, spin(b, 40), spin(c, -32)))
    for k in (5, 6, 7):
        j = 8 - k
        turn.append(jnp.where((at & 7) + j < 8, spin(turn[j], -j), spin(turn[j], 8 - j)))
    moments = jnp.zeros((NRHS, LANES), jnp.float32)
    for k in range(8):
        moments += jnp.where(
            (((lane - row) & 7) == k) & (lane < USED),
            jnp.broadcast_to(turn[k], (NRHS, LANES)),
            0.0,
        )
    return moments


def solve(table_ref, moments):
    lane = iota(1)
    rolled = [spin(moments, 8 * d) for d in ROLLS]
    a = []
    for j in range(DEPTH + 1):
        total = jnp.zeros((NRHS, LANES), jnp.float32)
        for k in range(len(ROLLS)):
            at = j * len(ROLLS) + k
            total += table_ref[at : at + 1, :] * rolled[k]
        a.append(total)
    right = a[DEPTH]
    for q in range(DEPTH):
        live = range(q, DEPTH + 1)
        col = [
            {j: jnp.broadcast_to(a[j][:, 8 * q + c : 8 * q + c + 1], (NRHS, LANES)) for j in live}
            for c in range(NRHS)
        ]
        for c in range(NRHS):
            k = 8 * q + c
            inverse = 1.0 / jnp.broadcast_to(col[c][q][c : c + 1], (NRHS, LANES))
            line = jnp.broadcast_to(a[q][c : c + 1], (NRHS, LANES)) * inverse
            for j in live:
                a[j] = jnp.where(lane == k, col[c][j] * inverse, a[j] - col[c][j] * line)
            for d in range(c + 1, NRHS):
                factor = jnp.broadcast_to(col[d][q][c : c + 1], (NRHS, LANES)) * inverse
                for j in live:
                    col[d][j] = col[d][j] - col[c][j] * factor
    return jnp.where(lane < DEPTH * NRHS, a[DEPTH], 0.0), right


def finish_kernel(table_ref, sums_ref, own_ref, v_ref, corr_ref, new_ref, est_ref):
    sums = sums_ref[0]
    for k in range(1, sums_ref.shape[0]):
        sums += sums_ref[k]
    moments = unpack(sums)
    lane, row = iota(1), iota(0)
    coeffs, right = solve(table_ref, moments)
    initial = jnp.sum(jnp.where(lane == row, moments, 0.0), 1, keepdims=True)
    gain = jnp.sum(right * coeffs, 1, keepdims=True)
    est = jnp.broadcast_to((initial - gain) / initial, (NRHS, LANES))
    est = jnp.sum(jnp.where(lane == row, est, 0.0), 0, keepdims=True)
    est_ref[...] = est[:, :NRHS]
    shift = jnp.zeros((NRHS, LANES), jnp.float32)
    for j in range(DEPTH):
        shift = jnp.where((lane >= 8 * j) & (lane < 8 * j + 8), SHIFTS[j], shift)
    kept = jnp.where(lane == row, 1.0, 0.0) - (shift * coeffs + SCALE_POWER * spin(coeffs, 8))
    high, middle, low = split(jnp.concatenate([coeffs, kept], 0))
    lane = lax.broadcasted_iota(jnp.int32, (2 * NRHS, LANES), 1)
    count = (DEPTH + 1) * NRHS
    middle_at = spin(middle, 3 * count)
    first = high + spin(high, count) + spin(high, 2 * count)
    first += jnp.where(lane >= 3 * count, middle_at, 0.0)
    second = jnp.where(lane < 4 * count - LANES, middle_at, 0.0)
    second += spin(middle, 4 * count) + spin(low, 5 * count)
    mix = jnp.concatenate([first, second], 1).astype(jnp.bfloat16)
    for x in range(CX):
        parts = []
        for y in range(CY):
            terms = [split(own_ref[x * CY + y])]
            terms += [split(v_ref[j, x * WY + DEPTH + y]) for j in range(DEPTH)]
            stack = [term[k] for k in (0, 1, 2, 0, 1, 0) for term in terms]
            stack += [jnp.zeros((NRHS, CZ), jnp.float32)] * 2
            w = jnp.concatenate(stack, 0).astype(jnp.bfloat16)
            parts.append(jnp.dot(mix, w, preferred_element_type=jnp.float32))
        both = jnp.stack(parts, 0)
        corr_ref[:, x] = jnp.swapaxes(both[:, :NRHS], 0, 1)
        new_ref[:, x] = jnp.swapaxes(both[:, NRHS:], 0, 1)


VMEM = pl.BlockSpec(memory_space=pltpu.VMEM)


def f32(*shape):
    return jax.ShapeDtypeStruct(shape, jnp.float32)


def call(kernel, specs, out_shape, *args, limit=12, flops=10**8, aliases=None):
    return pl.pallas_call(
        kernel,
        in_specs=specs,
        out_specs=jax.tree.map(lambda _: VMEM, out_shape),
        out_shape=out_shape,
        input_output_aliases=aliases or {},
        cost_estimate=pl.CostEstimate(flops=flops, bytes_accessed=10**6, transcendentals=0),
        compiler_params=pltpu.CompilerParams(vmem_limit_bytes=limit * 2**20),
    )(*args)


def swaps(count, odd):
    out = []
    for i in range(odd, count - 1, 2):
        out += [(i, i + 1), (i + 1, i)]
    return out


def exchanged(rows):
    count = lax.axis_size("gy")
    up = [(i, (i + 1) % count) for i in range(count)]
    down = [(target, source) for source, target in up]
    return lax.ppermute(rows[0], "gy", up), lax.ppermute(rows[1], "gy", down)


def first_of(axes, at):
    count = lax.axis_size(axes)
    return [[(at + i) % count for i in range(count)]]


def spread(x, axes, groups=None):
    count = lax.axis_size(axes)
    copies = jnp.broadcast_to(x[None], (count, *x.shape))
    return lax.all_to_all(copies, axes, 0, 0, tiled=True, axis_index_groups=groups)


def body(residual_block, diagonal):
    count_x = lax.axis_size(GX)
    raw = jnp.concatenate([residual_block, diagonal[None]], 0)
    odd = lax.ppermute(raw, GX, swaps(count_x, 1))
    even = lax.ppermute(raw, GX, swaps(count_x, 0))
    own, *near = call(pack_kernel, [VMEM], [f32(PACK, NRHS, CZ)] + [f32(NEXT, NRHS, CZ)] * 2, raw)
    near = exchanged(near)
    *rest, even, odd = call(side_kernel, [VMEM] * 2, [f32(REST, NRHS, CZ)] * 2 + [f32(PACK, NRHS, CZ)] * 2, even, odd)
    rest = exchanged(rest)
    state = [
        f32(DEPTH, WX * WY, NRHS, CZ),
        f32(DEPTH, CX * WY, NRHS, CZ),
        f32(WX * WY, NRHS, CZ),
    ]
    e, v, bc = call(inner_kernel, [VMEM] * 3, state, own, even, odd)
    e, v, bc, message = call(
        basis_kernel,
        [VMEM, (VMEM, VMEM), (VMEM, VMEM), VMEM, VMEM, VMEM],
        [*state, f32(1, MESSAGE)],
        own,
        (near[0], rest[0]),
        (near[1], rest[1]),
        e,
        v,
        bc,
        aliases={5: 0, 6: 1, 7: 2},
    )
    sums = spread(spread(message, NEAR, first_of(NEAR, 4)).sum(0), FAR, first_of(FAR, 8))
    corr, new, est = call(
        finish_kernel,
        [VMEM] * 4,
        [f32(*residual_block.shape), f32(*residual_block.shape), f32(1, NRHS)],
        jnp.asarray(roll_table()),
        sums,
        own,
        v,
    )
    return corr, new, est.reshape(NRHS)


def solution(mesh):
    split_mesh = Mesh(mesh.devices.reshape(16, 2, 4, mesh.shape["gy"]), ("z1", "z0", "y", "gy"))
    return jax.shard_map(
        body,
        mesh=split_mesh,
        in_specs=(P(None, GX, "gy", None), P(GX, "gy", None)),
        out_specs=(P(None, GX, "gy", None), P(None, GX, "gy", None), P()),
        check_vma=False,
    )
```
